32 devices in a mesh: dp: 8 (over y, x, core), mp: 4 (over z).
Axes of the slice: x: 2, y: 2, z: 4, core: 2. Of those that a mesh axis runs over, the one named last changes fastest.
Arguments:
- attn_out: bfloat16 [8192, 8192], P('dp', 'mp'), may hold values from -6 to 6
- out_weight: bfloat16 [8192, 8192], P('dp'), may hold values from -0.09375 to 0.09375
- residual: bfloat16 [8, 1024, 8192], P(None, 'mp', 'dp'), may hold values from -6 to 6
Outputs:
- layer_out: bfloat16 [8, 1024, 8192], P(None, 'mp', 'dp')
The draws below stay inside these ranges and needn't reach their ends.
All inputs are finite; a program needn't handle non-finite values.
Results may differ from the reference program's by a relative error of at most 0.001.
Values may be sent and summed in bfloat16 or wider, within the bound.
A program may use at most 192 MiB of HBM per device.

```python
import jax
import jax.numpy as jnp

D = 8192
TOK_DEV = 1024
HD = 8192
TOKENS = 8192
N_DP = 8


def with_spikes(array, stream_key, source, target, parts, factor):
    owner, partner = [(jnp.arange(array.shape[position]) // (array.shape[position] // parts)).reshape([-1 if axis == position else 1 for axis in range(array.ndim)]) for position in (source, target)]
    chosen = jax.random.permutation(stream_key, parts)[partner]
    strong = (owner == chosen) | (owner == (partner + parts // 2) % parts)
    return jnp.where(strong, factor * array, array)


def steps_of(stream_key, dims, pieces, least, high):
    def one(position, blocks):
        draws = jax.random.uniform(jax.random.fold_in(jax.random.fold_in(stream_key, 6), position), (blocks,), jnp.float32, least / len(pieces), high / len(pieces))
        return jnp.repeat(jnp.exp(draws), dims[position] // blocks).reshape((-1,) + (1,) * (len(dims) - position - 1))

    factor_of = one(*pieces[0])
    for cut in pieces[1:]:
        factor_of = factor_of * one(*cut)
    return factor_of


def bell_draw(key, dims, spread, reach, pieces=(), dtype=jnp.bfloat16):
    level = steps_of(key, dims, pieces, -0.22, 0.18) if pieces else 1.0
    entries = jax.random.normal(key, dims, jnp.float32) * spread * level
    return jnp.minimum(jnp.maximum(entries, -reach), reach).astype(dtype)


def noise_with(key, dims, scale, limit, split, heavy, held_as=jnp.bfloat16):
    entries = scale * jax.random.normal(key, dims, jnp.float32)
    if split:
        entries = entries * steps_of(key, dims, split, -0.22, 0.18)
    return jnp.clip(with_spikes(entries, jax.random.fold_in(key, 3), *heavy), -limit, limit).astype(held_as)


def setup_inputs(seed: int = 0) -> dict:
    splits = jax.random.split(jax.random.key(seed), 4)
    attn_out = bell_draw(splits[0], (TOKENS, HD), 1.0, 6.0, ((0, 8), (1, 4)))
    out_weight = noise_with(splits[1], (HD, D), HD ** -0.5, 0.09375, ((0, 8),), (0, 1, 8, 2.0))
    residual = bell_draw(splits[2], (N_DP, TOK_DEV, D), 1.0, 6.0, ((1, 4), (2, 8)))
    return {"attn_out": attn_out, "out_weight": out_weight, "residual": residual}


def reference(attn_out, out_weight, residual):
    projected = jnp.dot(attn_out, out_weight, preferred_element_type=jnp.float32)
    projected = projected.reshape(N_DP, TOK_DEV, D)
    return (residual.astype(jnp.float32) + projected).astype(jnp.bfloat16)
```

```python
import functools

import jax
import jax.numpy as jnp
from jax import lax
from jax.experimental import pallas as pl
from jax.experimental.pallas import tpu as pltpu
from jax.sharding import PartitionSpec as P

MESH = pl.DeviceIdType.MESH
CORES = 2
TILE = 16


def flip(index, mask):
    bit = 1
    while bit <= mask:
        if mask & bit:
            index = index + (1 - 2 * ((index // bit) % 2)) * bit
        bit *= 2
    return index


def shares_of(rows, planes):
    unit = rows // (4 * planes)
    counts = [unit] * planes
    counts[0] += (rows - unit * planes) // 2
    counts[-1] += rows - sum(counts)
    chunks, start = [], 0
    for count in counts:
        cut = (count // 2 + TILE - 1) // TILE * TILE if count > 2 * unit else count
        parts = [(start, cut)]
        if count > cut:
            parts.append((start + cut, count - cut))
        chunks.append(parts)
        start += count
    return chunks


def merged(first, second):
    out, a, b = [], list(first), list(second)
    total = max(len(a), len(b))
    for step in range(total):
        for tasks in (a, b):
            lo, hi = step * len(tasks) // total, (step + 1) * len(tasks) // total
            out.extend(tasks[lo:hi])
    return out


def gather_kernel(devices, planes, a_ref, w_ref, rows_ref, cols_ref, a_stage, w_stage,
                  az_s, az_r, ap_s, ap_r, ac_s, ac_r, wp_s, wp_r, wz_s, wz_r, loc):
    chips = devices // CORES
    tok, heads = a_ref.shape[0] // planes, a_ref.shape[1]
    depth, width = w_ref.shape[0], cols_ref.shape[1]
    half = tok // 2
    d = lax.axis_index("dp")
    z = lax.axis_index("mp")
    q, c = d // CORES, d % CORES
    chunks = shares_of(depth, planes)
    bits = [1 << k for k in range(chips.bit_length() - 1)]

    def chip_dev(mask, cross=0):
        return flip(q, mask) * CORES + flip(c, cross)

    def copy(src, dst, s, r, dp, mp):
        return pltpu.make_async_remote_copy(
            src_ref=src, dst_ref=dst, send_sem=s, recv_sem=r,
            device_id={"dp": dp, "mp": mp}, device_id_type=MESH)

    barrier = pltpu.get_barrier_semaphore()
    sources = [(m, x) for m in range(chips) for x in range(CORES) if (m, x) != (0, 0)]
    for m, x in sources:
        pl.semaphore_signal(barrier, inc=1, device_id={"dp": chip_dev(m, x), "mp": z}, device_id_type=MESH)
    for step in range(1, planes):
        pl.semaphore_signal(barrier, inc=1, device_id={"dp": d, "mp": lax.rem(z + step, planes)}, device_id_type=MESH)
    pl.semaphore_wait(barrier, len(sources) + planes - 1)

    def part(owner, j, h):
        return rows_ref.at[pl.ds(pl.multiple_of(owner * tok + h * half, TILE), half), pl.ds(j * heads, heads)]

    def wcols(dev):
        return pl.ds(pl.multiple_of(dev * width, 128), width)

    def wdst(dev, start, count):
        return cols_ref.at[pl.ds(pl.multiple_of(dev * depth + start, TILE), count), :]

    def run(me):
        sends, recvs = [], []

        def go(cp):
            cp.start()
            sends.append(cp)

        others = sorted((m for m in range(planes) if m != me), key=lambda m: -abs(m - me))
        for m in others:
            go(copy(a_ref.at[pl.ds(m * tok, tok), :],
                    rows_ref.at[pl.ds(pl.multiple_of(d * tok, TILE), tok), pl.ds(me * heads, heads)],
                    az_s.at[m], az_r.at[me], d, m))
        a_in = pltpu.make_async_copy(a_ref.at[pl.ds(me * tok, tok), :], a_stage, loc.at[0])
        w_in = pltpu.make_async_copy(w_ref.at[:, wcols(d)], w_stage, loc.at[1])
        a_in.start()
        w_in.start()

        nchunk = len(chunks[me])
        for k, (start, count) in enumerate(chunks[me]):
            for m, x in sources:
                if m:
                    to = chip_dev(m, x)
                    i = m * CORES + x
                    go(copy(w_ref.at[pl.ds(start, count), wcols(to)], wdst(d, start, count),
                            wp_s.at[i, k], wp_r.at[i, k], to, me))
        mate = chip_dev(0, 1)
        go(copy(w_ref.at[:, wcols(mate)], wdst(d, 0, depth), wp_s.at[1, 0], wp_r.at[1, 0], mate, me))

        def order(h):
            return bits if h == 0 else bits[::-1]

        def held_before(h, k):
            spans = [0]
            for bit in order(h)[:k]:
                spans += [u ^ bit for u in spans]
            return spans

        def to_mate(u, j, h, src=None):
            piece = part(chip_dev(u), j, h)
            go(copy(piece if src is None else src, piece, ac_s.at[u, j, h], ac_r.at[u, j, h], mate, me))

        def forward(u, j, h, k0, src=None):
            piece = part(chip_dev(u), j, h)
            for bit in order(h)[k0:]:
                go(copy(piece if src is None else src, piece, ap_s.at[u ^ bit, j, h], ap_r.at[u ^ bit, j, h],
                        chip_dev(bit), me))
            to_mate(u, j, h, src)

        for h in range(2):
            forward(0, me, h, 0, a_ref.at[pl.ds(me * tok + h * half, half), :])
        for j in others[::-1]:
            whole = rows_ref.at[pl.ds(pl.multiple_of(d * tok, TILE), tok), pl.ds(j * heads, heads)]
            copy(whole, whole, az_s.at[j], az_r.at[j], d, j).wait_recv()
            for h in range(2):
                forward(0, j, h, 0)

        def wait_w(sem, i, start, count, at):
            piece = wdst(chip_dev(i // CORES, i % CORES), start, count)
            copy(piece, piece, sem, sem, at, me).wait_recv()
            return piece

        def send_w(piece, origin, i, k, target):
            go(copy(piece, piece, wz_s.at[origin, i, k, int(target > me)], wz_r.at[origin, i, k], d, target))

        far = [m * CORES + x for m, x in sources if m]

        def share(k, i):
            start, count = chunks[me][k]
            piece = wait_w(wp_r.at[i, k], i, start, count, mate)
            for target in (me - 1, me + 1):
                if 0 <= target < planes:
                    send_w(piece, me, i, k, target)

        for k in range(nchunk):
            for i in far:
                share(k, i)

        def later(u, j, h, k0):
            piece = part(chip_dev(u), j, h)
            copy(piece, piece, ap_s.at[u, j, h], ap_r.at[u, j, h], mate, me).wait_recv()
            forward(u, j, h, k0)

        def pass_on(origin, i, k):
            start, count = chunks[origin][k]
            piece = wait_w(wz_r.at[origin, i, k], i, start, count, mate)
            target = me + (1 if origin < me else -1)
            if 0 <= target < planes:
                send_w(piece, origin, i, k, target)

        token_tasks = []
        js = [me] + others[::-1]
        for stage in range(len(bits)):
            for j in js:
                for h in range(2):
                    bit = order(h)[stage]
                    for u in held_before(h, stage):
                        token_tasks.append(functools.partial(later, u ^ bit, j, h, stage + 1))
        weight_tasks = []
        for dist in range(1, planes):
            origins = [o for o in (me - dist, me + dist) if 0 <= o < planes]
            for k in range(2):
                for i in far:
                    for o in origins:
                        if k < len(chunks[o]):
                            weight_tasks.append(functools.partial(pass_on, o, i, k))
        for task in merged(token_tasks, weight_tasks):
            task()

        a_in.wait()
        a_out = pltpu.make_async_copy(
            a_stage, rows_ref.at[pl.ds(pl.multiple_of(d * tok, TILE), tok), pl.ds(me * heads, heads)], loc.at[0])
        a_out.start()
        w_in.wait()
        w_out = pltpu.make_async_copy(w_stage, wdst(d, 0, depth), loc.at[1])
        w_out.start()
        piece = wdst(mate, 0, depth)
        copy(piece, piece, wp_s.at[1, 0], wp_r.at[1, 0], mate, me).wait_recv()
        for u in range(chips):
            for j in range(planes):
                for h in range(2):
                    piece = part(chip_dev(u, 1), j, h)
                    copy(piece, piece, ac_s.at[u, j, h], ac_r.at[u, j, h], mate, me).wait_recv()
        for cp in sends:
            cp.wait_send()
        a_out.wait()
        w_out.wait()

    for me in range(planes):
        pl.when(z == me)(functools.partial(run, me))


def shards(devices, planes, attn_out, out_weight, residual):
    chips = devices // CORES
    tok, heads = attn_out.shape[0] // planes, attn_out.shape[1]
    depth, width = out_weight.shape[0], out_weight.shape[1] // devices
    sem = pltpu.SemaphoreType.DMA
    rows, columns = pl.pallas_call(
        functools.partial(gather_kernel, devices, planes),
        out_shape=(
            jax.ShapeDtypeStruct((devices * tok, planes * heads), attn_out.dtype),
            jax.ShapeDtypeStruct((devices * depth, width), out_weight.dtype),
        ),
        in_specs=[pl.BlockSpec(memory_space=pl.ANY)] * 2,
        out_specs=[pl.BlockSpec(memory_space=pl.ANY)] * 2,
        scratch_shapes=[
            pltpu.VMEM((tok, heads), attn_out.dtype),
            pltpu.VMEM((depth, width), out_weight.dtype),
            sem((planes,)), sem((planes,)),
            sem((chips, planes, 2)), sem((chips, planes, 2)),
            sem((chips, planes, 2)), sem((chips, planes, 2)),
            sem((devices, 2)), sem((devices, 2)),
            sem((planes, devices, 2, 2)), sem((planes, devices, 2)),
            sem((2,)),
        ],
        compiler_params=pltpu.CompilerParams(collective_id=0, has_side_effects=True),
    )(attn_out, out_weight)
    projected = jnp.dot(rows, columns, preferred_element_type=jnp.float32)
    layer_out = residual.astype(jnp.float32) + projected.reshape(residual.shape)
    return layer_out.astype(jnp.bfloat16)


def solution(mesh):
    return jax.shard_map(
        functools.partial(shards, mesh.shape["dp"], mesh.shape["mp"]),
        mesh=mesh,
        in_specs=(P("dp", "mp"), P("dp", None), P(None, "mp", "dp")),
        out_specs=P(None, "mp", "dp"),
        check_vma=False,
    )
```

```python
import functools

import jax
import jax.numpy as jnp
from jax import lax
from jax.experimental import pallas as pl
from jax.experimental.pallas import tpu as pltpu
from jax.sharding import PartitionSpec as P

MESH = pl.DeviceIdType.MESH
CORES = 2
TILE = 16


def flip(index, mask):
    bit = 1
    while bit <= mask:
        if mask & bit:
            index = index + (1 - 2 * ((index // bit) % 2)) * bit
        bit *= 2
    return index


def shares_of(rows, planes):
    unit = rows // (4 * planes)
    counts = [unit] * planes
    counts[0] += (rows - unit * planes) // 2
    counts[-1] += rows - sum(counts)
    chunks, start = [], 0
    for count in counts:
        cut = (count // 2 + TILE - 1) // TILE * TILE if count > 2 * unit else count
        parts = [(start, cut)]
        if count > cut:
            parts.append((start + cut, count - cut))
        chunks.append(parts)
        start += count
    return chunks


def gather_kernel(devices, planes, a_ref, w_ref, rows_ref, cols_ref, a_stage, w_stage,
                  az_s, az_r, ap_s, ap_r, ac_s, ac_r, wp_s, wp_r, wz_s, wz_r, loc):
    chips = devices // CORES
    tok, heads = a_ref.shape[0] // planes, a_ref.shape[1]
    depth, width = w_ref.shape[0], cols_ref.shape[1]
    half = tok // 2
    d = lax.axis_index("dp")
    z = lax.axis_index("mp")
    q, c = d // CORES, d % CORES
    chunks = shares_of(depth, planes)
    bits = [1 << k for k in range(chips.bit_length() - 1)]

    def chip_dev(mask, cross=0):
        return flip(q, mask) * CORES + flip(c, cross)

    def copy(src, dst, s, r, dp, mp):
        return pltpu.make_async_remote_copy(
            src_ref=src, dst_ref=dst, send_sem=s, recv_sem=r,
            device_id={"dp": dp, "mp": mp}, device_id_type=MESH)

    barrier = pltpu.get_barrier_semaphore()
    sources = [(m, x) for m in range(chips) for x in range(CORES) if (m, x) != (0, 0)]
    for m, x in sources:
        pl.semaphore_signal(barrier, inc=1, device_id={"dp": chip_dev(m, x), "mp": z}, device_id_type=MESH)
    for step in range(1, planes):
        pl.semaphore_signal(barrier, inc=1, device_id={"dp": d, "mp": lax.rem(z + step, planes)}, device_id_type=MESH)
    pl.semaphore_wait(barrier, len(sources) + planes - 1)

    def part(owner, j, h):
        return rows_ref.at[pl.ds(pl.multiple_of(owner * tok + h * half, TILE), half), pl.ds(j * heads, heads)]

    def wcols(dev):
        return pl.ds(pl.multiple_of(dev * width, 128), width)

    def wdst(dev, start, count):
        return cols_ref.at[pl.ds(pl.multiple_of(dev * depth + start, TILE), count), :]

    def run(me):
        sends, recvs = [], []

        def go(cp):
            cp.start()
            sends.append(cp)

        others = sorted((m for m in range(planes) if m != me), key=lambda m: -abs(m - me))
        for m in others:
            go(copy(a_ref.at[pl.ds(m * tok, tok), :],
                    rows_ref.at[pl.ds(pl.multiple_of(d * tok, TILE), tok), pl.ds(me * heads, heads)],
                    az_s.at[m], az_r.at[me], d, m))
        a_in = pltpu.make_async_copy(a_ref.at[pl.ds(me * tok, tok), :], a_stage, loc.at[0])
        w_in = pltpu.make_async_copy(w_ref.at[:, wcols(d)], w_stage, loc.at[1])
        a_in.start()
        w_in.start()

        nchunk = len(chunks[me])
        for k, (start, count) in enumerate(chunks[me]):
            for m, x in sources:
                if m:
                    to = chip_dev(m, x)
                    i = m * CORES + x
                    go(copy(w_ref.at[pl.ds(start, count), wcols(to)], wdst(d, start, count),
                            wp_s.at[i, k], wp_r.at[i, k], to, me))
        mate = chip_dev(0, 1)
        go(copy(w_ref.at[:, wcols(mate)], wdst(d, 0, depth), wp_s.at[1, 0], wp_r.at[1, 0], mate, me))

        def order(h):
            return bits if h == 0 else bits[::-1]

        def held_before(h, k):
            spans = [0]
            for bit in order(h)[:k]:
                spans += [u ^ bit for u in spans]
            return spans

        def to_mate(u, j, h, src=None):
            piece = part(chip_dev(u), j, h)
            go(copy(piece if src is None else src, piece, ac_s.at[u, j, h], ac_r.at[u, j, h], mate, me))

        def forward(u, j, h, k0, src=None):
            piece = part(chip_dev(u), j, h)
            for bit in order(h)[k0:]:
                go(copy(piece if src is None else src, piece, ap_s.at[u ^ bit, j, h], ap_r.at[u ^ bit, j, h],
                        chip_dev(bit), me))
            to_mate(u, j, h, src)

        for h in range(2):
            forward(0, me, h, 0, a_ref.at[pl.ds(me * tok + h * half, half), :])
        share_of = [sum(count for _, count in parts) / depth for parts in chunks]
        wait_for = []

        def along(j):
            whole = rows_ref.at[pl.ds(pl.multiple_of(d * tok, TILE), tok), pl.ds(j * heads, heads)]
            copy(whole, whole, az_s.at[j], az_r.at[j], d, j).wait_recv()
            for h in range(2):
                forward(0, j, h, 0)

        line = planes if 0 < me < planes - 1 else planes - 1
        for rank, j in enumerate(others[::-1]):
            wait_for.append((line * (rank + 1) / len(others), functools.partial(along, j)))

        def wait_w(sem, i, start, count, at):
            piece = wdst(chip_dev(i // CORES, i % CORES), start, count)
            copy(piece, piece, sem, sem, at, me).wait_recv()
            return piece

        def send_w(piece, origin, i, k, target):
            go(copy(piece, piece, wz_s.at[origin, i, k, int(target > me)], wz_r.at[origin, i, k], d, target))

        far = [m * CORES + x for m, x in sources if m]

        def share(k, i):
            start, count = chunks[me][k]
            piece = wait_w(wp_r.at[i, k], i, start, count, mate)
            for target in (me - 1, me + 1):
                if 0 <= target < planes:
                    send_w(piece, me, i, k, target)

        inside = [(k, i) for k in range(nchunk) for i in far]
        fetched = 2 * planes * share_of[me]
        for p, (k, i) in enumerate(inside):
            wait_for.append((fetched * (p + 1) / len(inside), functools.partial(share, k, i)))

        def later(u, j, h, k0):
            piece = part(chip_dev(u), j, h)
            copy(piece, piece, ap_s.at[u, j, h], ap_r.at[u, j, h], mate, me).wait_recv()
            forward(u, j, h, k0)

        def pass_on(origin, i, k):
            start, count = chunks[origin][k]
            piece = wait_w(wz_r.at[origin, i, k], i, start, count, mate)
            target = me + (1 if origin < me else -1)
            if 0 <= target < planes:
                send_w(piece, origin, i, k, target)

        js = [me] + others[::-1]
        for stage in range(len(bits)):
            for rank, j in enumerate(js):
                for h in range(2):
                    bit = order(h)[stage]
                    for u in held_before(h, stage):
                        at = fetched + 1.5 * planes * (rank * 2 + h + 1) / (2 * len(js)) + 0.5 * stage
                        wait_for.append((at, functools.partial(later, u ^ bit, j, h, stage + 1)))
        for o in range(planes):
            if o != me:
                dist = abs(o - me)
                pieces = [(k, i) for k in range(len(chunks[o])) for i in far]
                first = planes - 1 if dist == 1 else planes + 3 * share_of[1]
                for p, (k, i) in enumerate(pieces):
                    at = first + 3 * planes * share_of[o] * (p + 1) / len(pieces) + 0.3 * dist
                    wait_for.append((at, functools.partial(pass_on, o, i, k)))
        for _, task in sorted(wait_for, key=lambda entry: entry[0]):
            task()

        a_in.wait()
        a_out = pltpu.make_async_copy(
            a_stage, rows_ref.at[pl.ds(pl.multiple_of(d * tok, TILE), tok), pl.ds(me * heads, heads)], loc.at[0])
        a_out.start()
        w_in.wait()
        w_out = pltpu.make_async_copy(w_stage, wdst(d, 0, depth), loc.at[1])
        w_out.start()
        piece = wdst(mate, 0, depth)
        copy(piece, piece, wp_s.at[1, 0], wp_r.at[1, 0], mate, me).wait_recv()
        for u in range(chips):
            for j in range(planes):
                for h in range(2):
                    piece = part(chip_dev(u, 1), j, h)
                    copy(piece, piece, ac_s.at[u, j, h], ac_r.at[u, j, h], mate, me).wait_recv()
        for cp in sends:
            cp.wait_send()
        a_out.wait()
        w_out.wait()

    for me in range(planes):
        pl.when(z == me)(functools.partial(run, me))


def shards(devices, planes, attn_out, out_weight, residual):
    chips = devices // CORES
    tok, heads = attn_out.shape[0] // planes, attn_out.shape[1]
    depth, width = out_weight.shape[0], out_weight.shape[1] // devices
    sem = pltpu.SemaphoreType.DMA
    rows, columns = pl.pallas_call(
        functools.partial(gather_kernel, devices, planes),
        out_shape=(
            jax.ShapeDtypeStruct((devices * tok, planes * heads), attn_out.dtype),
            jax.ShapeDtypeStruct((devices * depth, width), out_weight.dtype),
        ),
        in_specs=[pl.BlockSpec(memory_space=pl.ANY)] * 2,
        out_specs=[pl.BlockSpec(memory_space=pl.ANY)] * 2,
        scratch_shapes=[
            pltpu.VMEM((tok, heads), attn_out.dtype),
            pltpu.VMEM((depth, width), out_weight.dtype),
            sem((planes,)), sem((planes,)),
            sem((chips, planes, 2)), sem((chips, planes, 2)),
            sem((chips, planes, 2)), sem((chips, planes, 2)),
            sem((devices, 2)), sem((devices, 2)),
            sem((planes, devices, 2, 2)), sem((planes, devices, 2)),
            sem((2,)),
        ],
        compiler_params=pltpu.CompilerParams(collective_id=0, has_side_effects=True),
    )(attn_out, out_weight)
    projected = jnp.dot(rows, columns, preferred_element_type=jnp.float32)
    layer_out = residual.astype(jnp.float32) + projected.reshape(residual.shape)
    return layer_out.astype(jnp.bfloat16)


def solution(mesh):
    return jax.shard_map(
        functools.partial(shards, mesh.shape["dp"], mesh.shape["mp"]),
        mesh=mesh,
        in_specs=(P("dp", "mp"), P("dp", None), P(None, "mp", "dp")),
        out_specs=P(None, "mp", "dp"),
        check_vma=False,
    )
```

```python
import functools

import jax
import jax.numpy as jnp
from jax import lax
from jax.experimental import pallas as pl
from jax.experimental.pallas import tpu as pltpu
from jax.sharding import PartitionSpec as P

MESH = pl.DeviceIdType.MESH
CORES = 2
TILE = 16


def flip(index, mask):
    bit = 1
    while bit <= mask:
        if mask & bit:
            index = index + (1 - 2 * ((index // bit) % 2)) * bit
        bit *= 2
    return index


def shares_of(rows, planes):
    unit = rows // (4 * planes)
    counts = [unit] * planes
    counts[0] += (rows - unit * planes) // 2
    counts[-1] += rows - sum(counts)
    chunks, start = [], 0
    for count in counts:
        cut = (count // 2 + TILE - 1) // TILE * TILE if count > 2 * unit else count
        parts = [(start, cut)]
        if count > cut:
            parts.append((start + cut, count - cut))
        chunks.append(parts)
        start += count
    return chunks


def gather_kernel(devices, planes, a_ref, w_ref, rows_ref, cols_ref, a_stage, w_stage,
                  az_s, az_r, ap_s, ap_r, ac_s, ac_r, wp_s, wp_r, wz_s, wz_r, loc):
    chips = devices // CORES
    tok, heads = a_ref.shape[0] // planes, a_ref.shape[1]
    depth, width = w_ref.shape[0], cols_ref.shape[1]
    half = tok // 2
    d = lax.axis_index("dp")
    z = lax.axis_index("mp")
    q, c = d // CORES, d % CORES
    chunks = shares_of(depth, planes)
    bits = [1 << k for k in range(chips.bit_length() - 1)]

    def chip_dev(mask, cross=0):
        return flip(q, mask) * CORES + flip(c, cross)

    def copy(src, dst, s, r, dp, mp):
        return pltpu.make_async_remote_copy(
            src_ref=src, dst_ref=dst, send_sem=s, recv_sem=r,
            device_id={"dp": dp, "mp": mp}, device_id_type=MESH)

    barrier = pltpu.get_barrier_semaphore()
    sources = [(m, x) for m in range(chips) for x in range(CORES) if (m, x) != (0, 0)]
    for m, x in sources:
        pl.semaphore_signal(barrier, inc=1, device_id={"dp": chip_dev(m, x), "mp": z}, device_id_type=MESH)
    for step in range(1, planes):
        pl.semaphore_signal(barrier, inc=1, device_id={"dp": d, "mp": lax.rem(z + step, planes)}, device_id_type=MESH)
    pl.semaphore_wait(barrier, len(sources) + planes - 1)

    def part(owner, j, h):
        return rows_ref.at[pl.ds(pl.multiple_of(owner * tok + h * half, TILE), half), pl.ds(j * heads, heads)]

    def wcols(dev):
        return pl.ds(pl.multiple_of(dev * width, 128), width)

    def wdst(dev, start, count):
        return cols_ref.at[pl.ds(pl.multiple_of(dev * depth + start, TILE), count), :]

    def run(me):
        sends, recvs = [], []

        def go(cp):
            cp.start()
            sends.append(cp)

        others = sorted((m for m in range(planes) if m != me), key=lambda m: abs(m - me))
        for m in others:
            for h in range(2):
                go(copy(a_ref.at[pl.ds(m * tok + h * half, half), :], part(d, me, h),
                        az_s.at[m, h], az_r.at[me, h], d, m))
        a_in = pltpu.make_async_copy(a_ref.at[pl.ds(me * tok, tok), :], a_stage, loc.at[0])
        w_in = pltpu.make_async_copy(w_ref.at[:, wcols(d)], w_stage, loc.at[1])
        a_in.start()
        w_in.start()

        nchunk = len(chunks[me])
        for k, (start, count) in enumerate(chunks[me]):
            for m, x in sources:
                if m:
                    to = chip_dev(m, x)
                    i = m * CORES + x
                    go(copy(w_ref.at[pl.ds(start, count), wcols(to)], wdst(d, start, count),
                            wp_s.at[i, k], wp_r.at[i, k], to, me))
        mate = chip_dev(0, 1)
        go(copy(w_ref.at[:, wcols(mate)], wdst(d, 0, depth), wp_s.at[1, 0], wp_r.at[1, 0], mate, me))

        def order(h):
            return bits if h == 0 else bits[::-1]

        def held_before(h, k):
            spans = [0]
            for bit in order(h)[:k]:
                spans += [u ^ bit for u in spans]
            return spans

        def to_mate(u, j, h, src=None):
            piece = part(chip_dev(u), j, h)
            go(copy(piece if src is None else src, piece, ac_s.at[u, j, h], ac_r.at[u, j, h], mate, me))

        def forward(u, j, h, k0, src=None):
            piece = part(chip_dev(u), j, h)
            for bit in order(h)[k0:]:
                go(copy(piece if src is None else src, piece, ap_s.at[u ^ bit, j, h], ap_r.at[u ^ bit, j, h],
                        chip_dev(bit), me))
            to_mate(u, j, h, src)

        for h in range(2):
            forward(0, me, h, 0, a_ref.at[pl.ds(me * tok + h * half, half), :])
        share_of = [sum(count for _, count in parts) / depth for parts in chunks]
        wait_for = []

        def along(j, h):
            piece = part(d, j, h)
            copy(piece, piece, az_s.at[j, h], az_r.at[j, h], d, j).wait_recv()
            forward(0, j, h, 0)

        line = planes if 0 < me < planes - 1 else planes - 1
        for rank, j in enumerate(others):
            for h in range(2):
                at = line * (rank + 0.5 * (h + 1)) / len(others)
                wait_for.append((at, functools.partial(along, j, h)))

        def wait_w(sem, i, start, count, at):
            piece = wdst(chip_dev(i // CORES, i % CORES), start, count)
            copy(piece, piece, sem, sem, at, me).wait_recv()
            return piece

        def send_w(piece, origin, i, k, target):
            go(copy(piece, piece, wz_s.at[origin, i, k, int(target > me)], wz_r.at[origin, i, k], d, target))

        far = [m * CORES + x for m, x in sources if m]

        def share(k, i):
            start, count = chunks[me][k]
            piece = wait_w(wp_r.at[i, k], i, start, count, mate)
            for target in (me - 1, me + 1):
                if 0 <= target < planes:
                    send_w(piece, me, i, k, target)

        inside = [(k, i) for k in range(nchunk) for i in far]
        fetched = 2 * planes * share_of[me]
        for p, (k, i) in enumerate(inside):
            wait_for.append((fetched * (p + 1) / len(inside), functools.partial(share, k, i)))

        def later(u, j, h, k0):
            piece = part(chip_dev(u), j, h)
            copy(piece, piece, ap_s.at[u, j, h], ap_r.at[u, j, h], mate, me).wait_recv()
            forward(u, j, h, k0)

        def pass_on(origin, i, k):
            start, count = chunks[origin][k]
            piece = wait_w(wz_r.at[origin, i, k], i, start, count, mate)
            target = me + (1 if origin < me else -1)
            if 0 <= target < planes:
                send_w(piece, origin, i, k, target)

        js = [me] + others
        for stage in range(len(bits)):
            for rank, j in enumerate(js):
                for h in range(2):
                    bit = order(h)[stage]
                    for u in held_before(h, stage):
                        at = fetched + 1.5 * planes * (rank * 2 + h + 1) / (2 * len(js)) + 0.5 * stage
                        wait_for.append((at, functools.partial(later, u ^ bit, j, h, stage + 1)))
        for o in range(planes):
            if o != me:
                dist = abs(o - me)
                pieces = [(k, i) for k in range(len(chunks[o])) for i in far]
                first = planes - 1 if dist == 1 else planes + 3 * share_of[1]
                for p, (k, i) in enumerate(pieces):
                    at = first + 3 * planes * share_of[o] * (p + 1) / len(pieces) + 0.3 * dist
                    wait_for.append((at, functools.partial(pass_on, o, i, k)))
        for _, task in sorted(wait_for, key=lambda entry: entry[0]):
            task()

        a_in.wait()
        a_out = pltpu.make_async_copy(
            a_stage, rows_ref.at[pl.ds(pl.multiple_of(d * tok, TILE), tok), pl.ds(me * heads, heads)], loc.at[0])
        a_out.start()
        w_in.wait()
        w_out = pltpu.make_async_copy(w_stage, wdst(d, 0, depth), loc.at[1])
        w_out.start()
        piece = wdst(mate, 0, depth)
        copy(piece, piece, wp_s.at[1, 0], wp_r.at[1, 0], mate, me).wait_recv()
        for u in range(chips):
            for j in range(planes):
                for h in range(2):
                    piece = part(chip_dev(u, 1), j, h)
                    copy(piece, piece, ac_s.at[u, j, h], ac_r.at[u, j, h], mate, me).wait_recv()
        for cp in sends:
            cp.wait_send()
        a_out.wait()
        w_out.wait()

    for me in range(planes):
        pl.when(z == me)(functools.partial(run, me))


def shards(devices, planes, attn_out, out_weight, residual):
    chips = devices // CORES
    tok, heads = attn_out.shape[0] // planes, attn_out.shape[1]
    depth, width = out_weight.shape[0], out_weight.shape[1] // devices
    sem = pltpu.SemaphoreType.DMA
    rows, columns = pl.pallas_call(
        functools.partial(gather_kernel, devices, planes),
        out_shape=(
            jax.ShapeDtypeStruct((devices * tok, planes * heads), attn_out.dtype),
            jax.ShapeDtypeStruct((devices * depth, width), out_weight.dtype),
        ),
        in_specs=[pl.BlockSpec(memory_space=pl.ANY)] * 2,
        out_specs=[pl.BlockSpec(memory_space=pl.ANY)] * 2,
        scratch_shapes=[
            pltpu.VMEM((tok, heads), attn_out.dtype),
            pltpu.VMEM((depth, width), out_weight.dtype),
            sem((planes, 2)), sem((planes, 2)),
            sem((chips, planes, 2)), sem((chips, planes, 2)),
            sem((chips, planes, 2)), sem((chips, planes, 2)),
            sem((devices, 2)), sem((devices, 2)),
            sem((planes, devices, 2, 2)), sem((planes, devices, 2)),
            sem((2,)),
        ],
        compiler_params=pltpu.CompilerParams(collective_id=0, has_side_effects=True),
    )(attn_out, out_weight)
    projected = jnp.dot(rows, columns, preferred_element_type=jnp.float32)
    layer_out = residual.astype(jnp.float32) + projected.reshape(residual.shape)
    return layer_out.astype(jnp.bfloat16)


def solution(mesh):
    return jax.shard_map(
        functools.partial(shards, mesh.shape["dp"], mesh.shape["mp"]),
        mesh=mesh,
        in_specs=(P("dp", "mp"), P("dp", None), P(None, "mp", "dp")),
        out_specs=P(None, "mp", "dp"),
        check_vma=False,
    )
```
